256 devices in a mesh: dp: 16 (over y, x), row: 16 (over z, core).
Axes of the slice: x: 4, y: 4, z: 8, core: 2. Of those that a mesh axis runs over, the one named last changes fastest.
Arguments:
- bag_index: int32 [131072, 16], P(('dp', 'row')), may hold values from 0 to 9215, as said below
- pooled_grad: bfloat16 [131072, 256], P(('dp', 'row')), may hold values from -6 to 6
- touched_ids: int32 [256, 1024], P(('dp', 'row')), may hold values from 0 to 1023, as said below
- owner_counts: int32 [256, 256], P(('dp', 'row')), may hold values from 1 to 8, as said below
- cold_table: float32 [262144, 256], P(('dp', 'row')), may hold values from -6 to 6
- cold_moment_codes: bfloat16 [262144, 256], P(('dp', 'row')), may hold values from -1 to 1
- cold_second_codes: bfloat16 [262144, 256], P(('dp', 'row')), may hold values from 0.049804688 to 1
- cold_moment_scales: float32 [262144], P(('dp', 'row')), may hold values from 0.05 to 2
- cold_second_scales: float32 [262144], P(('dp', 'row')), may hold values from 0.01 to 1
- hot_table: float32 [8192, 256], replicated, may hold values from -6 to 6
- hot_moment_codes: bfloat16 [8192, 256], P('row'), may hold values from -1 to 1
- hot_second_codes: bfloat16 [8192, 256], P('row'), may hold values from 0.049804688 to 1
- hot_moment_scales: float32 [8192], P('row'), may hold values from 0.05 to 2
- hot_second_scales: float32 [8192], P('row'), may hold values from 0.01 to 1
Outputs:
- cold_table_new: float32 [262144, 256], P(('dp', 'row'))
- cold_moment_codes_new: bfloat16 [262144, 256], P(('dp', 'row'))
- cold_second_codes_new: bfloat16 [262144, 256], P(('dp', 'row'))
- cold_moment_scales_new: float32 [262144], P(('dp', 'row'))
- cold_second_scales_new: float32 [262144], P(('dp', 'row'))
- hot_replica: float32 [8192, 256], replicated
- hot_moment_codes_new: bfloat16 [8192, 256], P('row')
- hot_second_codes_new: bfloat16 [8192, 256], P('row')
- hot_moment_scales_new: float32 [8192], P('row')
- hot_second_scales_new: float32 [8192], P('row')
The draws below stay inside these ranges and needn't reach their ends.
Inputs may be any that keep to these rules, and one draw needn't show every extreme that they name: `bag_index`: each device's rows of samples name every value below 1024 at least once; a value v of 1024 or more names hot row v - 1024. `owner_counts`: row k belongs to device k; its entries, one for each owning device in order along dp then row, sum to 1024; some owner gets 8 from every device. `touched_ids`: row k lists device k's touched rows grouped by owner in owner order, owner o's group holding owner_counts[k, o] entries; entries within a group are distinct.
All inputs are finite; a program needn't handle non-finite values.
Results may differ from the reference program's by a relative error of at most 0.001.
Values may be sent and summed in bfloat16 or wider, within the bound.
A program may use at most 128 MiB of HBM per device.

```python
import math
import jax
import jax.numpy as jnp
from jax import lax

E = 256
POOL = 16
CAP = 8
OWN = 1024
SAMP_DEV = 512
OWNERS = 256
TOUCH_DEV = 1024
HOT = 8192
SLAB = 262144
SAMPLES = 131072
N_DP = 16
N_ROW = 16


def touch_layout(key):
    owners = OWNERS
    key_list = jax.random.split(jax.random.fold_in(key, 71), 4)
    full_owner = jax.random.randint(key_list[0], (), 0, owners)
    cell_count = (owners - 1) * (CAP - 1)
    spare_units = TOUCH_DEV - CAP - (owners - 1)
    ranking = jax.vmap(lambda subkey: jax.random.permutation(subkey, cell_count))(jax.random.split(key_list[1], owners))
    chosen = (ranking < spare_units).astype(jnp.int32).reshape(owners, owners - 1, CAP - 1)
    others = 1 + jnp.sum(chosen, axis=2)
    shifted = jnp.concatenate([jnp.full((owners, 1), CAP, jnp.int32), others.astype(jnp.int32)], axis=1)
    offset = (jnp.arange(owners, dtype=jnp.int32) - full_owner) % owners
    counts = shifted[:, offset].astype(jnp.int32)
    run_end = jnp.cumsum(counts, axis=1).astype(jnp.int32)
    starts = run_end - counts
    positions = jnp.arange(TOUCH_DEV, dtype=jnp.int32)
    owner_of = jax.vmap(lambda limits: jnp.searchsorted(limits, positions, side='right'))(run_end).astype(jnp.int32)
    within = positions[None, :] - jnp.take_along_axis(starts, owner_of, axis=1)
    base_offset = jax.random.randint(key_list[2], (owners, owners), 0, OWN)
    shuffle = jax.vmap(lambda subkey: jax.random.permutation(subkey, OWN))(jax.random.split(key_list[3], owners))
    slot_index = (jnp.take_along_axis(base_offset, owner_of, axis=1) + within) % OWN
    row_ids = jnp.take_along_axis(shuffle, slot_index.astype(jnp.int32), axis=1)
    return (counts, row_ids.astype(jnp.int32))


def draw_owner_counts(key, part):
    return touch_layout(key)[0]


def draw_touched_ids(key, part):
    return touch_layout(key)[1]


def draw_bag_index(key, part):
    owners = OWNERS
    entries = SAMP_DEV * POOL
    key_list = jax.random.split(jax.random.fold_in(key, 13), 6)
    hot_order = jax.random.permutation(key_list[0], HOT).astype(jnp.int32)
    ranking = jax.vmap(lambda subkey: jax.random.permutation(subkey, entries))(jax.random.split(key_list[1], owners)).astype(jnp.int32)
    cold_pick = jax.random.randint(key_list[2], (owners, entries), 0, TOUCH_DEV)
    coin_flip = jax.random.randint(key_list[3], (owners, entries), 0, 2)
    first_factor = jax.random.randint(key_list[4], (owners, entries), 0, HOT)
    second_factor = jax.random.randint(key_list[5], (owners, entries), 0, HOT)
    hot_pick = hot_order[first_factor * second_factor // HOT]
    values = jnp.where(ranking < TOUCH_DEV, ranking, jnp.where(coin_flip == 1, TOUCH_DEV + hot_pick, cold_pick))
    return values.reshape(owners * SAMP_DEV, POOL).astype(jnp.int32)


def block_scale(own_key, shape, pieces, least, top_value):
    gain, own = 1.0, jax.random.fold_in(own_key, 6)
    for position, blocks in pieces:
        heights = jnp.exp(jax.random.uniform(jax.random.fold_in(own, position), (blocks,), jnp.float32, least / len(pieces), top_value / len(pieces)))
        gain = gain * jnp.repeat(heights, shape[position] // blocks).reshape([-1 if axis == position else 1 for axis in range(len(shape))])
    return gain


def normal_values(stream_key, shape, width, reach, pieces=(), held_as=jnp.bfloat16):
    factor_of = block_scale(stream_key, shape, pieces, -0.22, 0.18) if pieces else 1.0
    array = jax.random.normal(stream_key, shape, jnp.float32) * width * factor_of
    return jnp.minimum(jnp.maximum(array, -reach), reach).astype(held_as)


def setup_inputs(seed: int = 0) -> dict:
    streams_of = jax.random.split(jax.random.key(seed), 15)
    return {
        "bag_index": draw_bag_index(jax.random.fold_in(streams_of[14], 71), 0),
        "pooled_grad": normal_values(streams_of[1], (SAMPLES, E), 1.0, 6.0, ((0, 256),)),
        "touched_ids": draw_touched_ids(jax.random.fold_in(streams_of[14], 71), 0),
        "owner_counts": draw_owner_counts(jax.random.fold_in(streams_of[14], 71), 0),
        "cold_table": normal_values(streams_of[4], (SLAB, E), 1.0, 6.0, ((0, 256),), jnp.float32),
        "cold_moment_codes": jnp.clip(jax.random.uniform(streams_of[5], (SLAB, E), jnp.float32, -1.0, 1.0) * block_scale(streams_of[5], (SLAB, E), ((0, 256),), -0.4, 0.0), -1.0, 1.0).astype(jnp.bfloat16),
        "cold_second_codes": jnp.clip(0.049804688 + 0.9501953 * jax.random.uniform(streams_of[6], (SLAB, E), jnp.float32) ** block_scale(streams_of[6], (SLAB, E), ((0, 256),), -0.2, 0.2), 0.049804688, 1.0).astype(jnp.bfloat16),
        "cold_moment_scales": jnp.clip(jnp.exp(math.log(2.0) - 3.6888794 * jax.random.uniform(streams_of[7], (SLAB,), jnp.float32) ** block_scale(streams_of[7], (SLAB,), ((0, 256),), -0.2, 0.2)), 0.05, 2.0),
        "cold_second_scales": jnp.clip(jnp.exp(math.log(1.0) - 4.6051702 * jax.random.uniform(streams_of[8], (SLAB,), jnp.float32) ** block_scale(streams_of[8], (SLAB,), ((0, 256),), -0.2, 0.2)), 0.01, 1.0),
        "hot_table": normal_values(streams_of[9], (HOT, E), 1.0, 6.0, (), jnp.float32),
        "hot_moment_codes": jnp.clip(jax.random.uniform(streams_of[10], (HOT, E), jnp.float32, -1.0, 1.0) * block_scale(streams_of[10], (HOT, E), ((0, 16),), -0.4, 0.0), -1.0, 1.0).astype(jnp.bfloat16),
        "hot_second_codes": jnp.clip(0.049804688 + 0.9501953 * jax.random.uniform(streams_of[11], (HOT, E), jnp.float32) ** block_scale(streams_of[11], (HOT, E), ((0, 16),), -0.2, 0.2), 0.049804688, 1.0).astype(jnp.bfloat16),
        "hot_moment_scales": jnp.clip(jnp.exp(math.log(2.0) - 3.6888794 * jax.random.uniform(streams_of[12], (HOT,), jnp.float32) ** block_scale(streams_of[12], (HOT,), ((0, 16),), -0.2, 0.2)), 0.05, 2.0),
        "hot_second_scales": jnp.clip(jnp.exp(math.log(1.0) - 4.6051702 * jax.random.uniform(streams_of[13], (HOT,), jnp.float32) ** block_scale(streams_of[13], (HOT,), ((0, 16),), -0.2, 0.2)), 0.01, 1.0),
    }


beta_one = 0.9
beta_two = 0.999
learn_rate = 0.1
adam_eps = 1e-08
bias_one = 1.0 - 1.7478712517226947e-46
bias_two = 0.6323045752290363

def adam_rows(weights, moment_codes, second_codes, moment_scales, second_scales, gradient):
    moment = beta_one * moment_scales[:, None] * moment_codes.astype(jnp.float32) + (1.0 - beta_one) * gradient
    second = beta_two * second_scales[:, None] * second_codes.astype(jnp.float32) + (1.0 - beta_two) * gradient * gradient
    updated = weights - learn_rate * (moment / bias_one) / (jnp.sqrt(second / bias_two) + adam_eps)
    moment_scale_new = lax.optimization_barrier(jnp.max(jnp.abs(moment), axis=1)) + 1e-06
    second_scale_new = lax.optimization_barrier(jnp.max(second, axis=1)) + 1e-06
    moment_code_new = (moment / moment_scale_new[:, None]).astype(jnp.bfloat16)
    second_code_new = (second / second_scale_new[:, None]).astype(jnp.bfloat16)
    return (updated, moment_code_new, second_code_new, moment_scale_new, second_scale_new)

def reference(bag_index, pooled_grad, touched_ids, owner_counts, cold_table, cold_moment_codes, cold_second_codes, cold_moment_scales, cold_second_scales, hot_table, hot_moment_codes, hot_second_codes, hot_moment_scales, hot_second_scales):
    owners = N_DP * N_ROW
    local_rows = TOUCH_DEV + HOT
    bags_split = bag_index.reshape(owners, SAMP_DEV, POOL)
    grads_split = pooled_grad.reshape(owners, SAMP_DEV, E)
    positions = jnp.arange(TOUCH_DEV, dtype=jnp.int32)
    columns = jnp.arange(local_rows, dtype=jnp.int32)

    def visit(carry, inputs):
        cold_sum, hot_sum = carry
        bag_rows, grad_rows, id_row, count_row = inputs
        tally = jnp.zeros((SAMP_DEV, local_rows), jnp.float32)
        for entry in range(POOL):
            tally = tally + (bag_rows[:, entry][:, None] == columns[None, :]).astype(jnp.float32)
        local_grad = jnp.dot(tally.T.astype(jnp.bfloat16), grad_rows, preferred_element_type=jnp.float32)
        run_end = jnp.cumsum(count_row).astype(jnp.int32)
        owner = lax.optimization_barrier(jnp.sum((run_end[None, :] <= positions[:, None]).astype(jnp.int32), axis=1)).astype(jnp.int32)
        target = (owner * OWN + id_row).astype(jnp.int32)
        cold_sum = cold_sum.at[target].add(local_grad[:TOUCH_DEV])
        hot_sum = hot_sum + local_grad[TOUCH_DEV:]
        return ((cold_sum, hot_sum), None)
    start = (jnp.zeros((owners * OWN, E), jnp.float32), jnp.zeros((HOT, E), jnp.float32))
    (cold_grad, hot_grad), _ = lax.scan(visit, start, (bags_split, grads_split, touched_ids, owner_counts))
    cold = adam_rows(cold_table, cold_moment_codes, cold_second_codes, cold_moment_scales, cold_second_scales, cold_grad)
    hot = adam_rows(hot_table, hot_moment_codes, hot_second_codes, hot_moment_scales, hot_second_scales, hot_grad)
    return (cold[0], cold[1], cold[2], cold[3], cold[4], hot[0], hot[1], hot[2], hot[3], hot[4])
```

```python
import functools

import jax
import jax.numpy as jnp
from jax import lax
from jax.experimental import pallas as pl
from jax.experimental.pallas import tpu as pltpu
from jax.sharding import PartitionSpec as P

CAP = 8
beta_one = 0.9
beta_two = 0.999
learn_rate = 0.1
adam_eps = 1e-08
bias_one = 1.0 - 1.7478712517226947e-46
bias_two = 0.6323045752290363

MESH = pl.DeviceIdType.MESH
F32 = jnp.float32
BF16 = jnp.bfloat16
I32 = jnp.int32
NIBBLES = 0x0F0F0F0F


def adam_parts(codes_m, codes_s, scale_m, scale_s, grad):
    moment = beta_one * scale_m * codes_m.astype(F32) + (1.0 - beta_one) * grad
    second = beta_two * scale_s * codes_s.astype(F32) + (1.0 - beta_two) * grad * grad
    update = learn_rate * (moment / bias_one) / (jnp.sqrt(second / bias_two) + adam_eps)
    new_m = jnp.max(jnp.abs(moment), axis=1, keepdims=True) + 1e-06
    new_s = jnp.max(second, axis=1, keepdims=True) + 1e-06
    return (
        update,
        (moment / new_m).astype(BF16),
        (second / new_s).astype(BF16),
        new_m,
        new_s,
    )


def lanes_to_column(line, rows, first):
    shape = (rows, line.shape[1])
    at = lax.broadcasted_iota(I32, shape, 1) == lax.broadcasted_iota(I32, shape, 0) + first
    return jnp.sum(jnp.where(at, jnp.broadcast_to(line, shape), 0.0), axis=1, keepdims=True)


def column_to_lanes(column, lanes):
    shape = (column.shape[0], lanes)
    at = lax.broadcasted_iota(I32, shape, 1) == lax.broadcasted_iota(I32, shape, 0)
    return jnp.sum(jnp.where(at, jnp.broadcast_to(column, shape), 0.0), axis=0, keepdims=True)


def exchange_kernel(
    n_dp,
    n_row,
    pool_ref,
    note_ref,
    codes_m_ref,
    codes_s_ref,
    scale_m_ref,
    scale_s_ref,
    cold_in,
    ids_in,
    steps_q,
    steps_scale,
    new_m_ref,
    new_s_ref,
    lines_ref,
    pools,
    notes,
    tally,
    hot_sum,
    cold_out,
    ids_out,
    hot_in,
    line_out,
    pool_sems,
    note_sems,
    step_sems,
    step_scale_sems,
    bulk_sems,
    local_sems,
):
    d = lax.axis_index("dp")
    r = lax.axis_index("row")
    chips = n_row // 2
    z, c = r // 2, r % 2
    sign = 1 - 2 * c
    half = pool_ref.shape[0] // 2
    block = hot_sum.shape[0]
    piece = block // n_dp
    slots = n_dp * CAP
    main_hops, other_hops = chips // 2, chips // 2 - 1

    def row_of(chip, core):
        return lax.rem(chip + 2 * chips, chips) * 2 + core

    main_to = row_of(z + sign, c)
    other_to = row_of(z - sign, c)
    sibling = row_of(z, 1 - c)

    def peer(i):
        return lax.rem(d + i, n_dp)

    own = pltpu.make_async_copy(pool_ref, pools.at[r], local_sems.at[0])
    own_note = pltpu.make_async_copy(note_ref, notes.at[r], local_sems.at[1])
    own.start()
    own_note.start()

    barrier = pltpu.get_barrier_semaphore()
    for to in (main_to, other_to, sibling):
        pl.semaphore_signal(barrier, inc=1, device_id=(d, to), device_id_type=MESH)

    def greet(i, carry):
        pl.semaphore_signal(barrier, inc=1, device_id=(peer(i), r), device_id_type=MESH)
        return carry

    lax.fori_loop(1, n_dp, greet, 0)
    own.wait()
    own_note.wait()
    hot_sum[...] = jnp.zeros_like(hot_sum)
    pl.semaphore_wait(barrier, n_dp + 2)

    def ring(big, small, big_sems, small_sems, use):
        span = big.shape[1] // 2

        def copies(source, b, to, lane, k):
            at = big.at[source, pl.ds(b * span, span)]
            n = k * 2 + b
            yield pltpu.make_async_remote_copy(
                src_ref=at,
                dst_ref=at,
                send_sem=big_sems.at[2 * lane, n],
                recv_sem=big_sems.at[2 * lane + 1, n],
                device_id=(d, to),
                device_id_type=MESH,
            )

        def note(source, to, lane, k):
            return pltpu.make_async_remote_copy(
                src_ref=small.at[source],
                dst_ref=small.at[source],
                send_sem=small_sems.at[2 * lane, k],
                recv_sem=small_sems.at[2 * lane + 1, k],
                device_id=(d, to),
                device_id_type=MESH,
            )

        def send(source, b, to, lane, k):
            if b == 0:
                note(source, to, lane, k).start()
            for copy in copies(source, b, to, lane, k):
                copy.start()

        def arrive(source, b, to, lane, k):
            if b == 0:
                note(source, to, lane, k).wait_recv()
            for copy in copies(source, b, to, lane, k):
                copy.wait_recv()

        def sent(source, b, to, lane, k):
            if b == 0:
                note(source, to, lane, k).wait_send()
            for copy in copies(source, b, to, lane, k):
                copy.wait_send()

        def step(k, carry):
            from_main = row_of(z - sign * k, c)
            from_other = row_of(z + sign * k, c)
            has_other = jnp.logical_and(k >= 1, k <= other_hops)
            for b in range(2):

                @pl.when(k >= 1)
                def _():
                    arrive(from_main, b, main_to, 0, k - 1)

                @pl.when(k < main_hops)
                def _():
                    send(from_main, b, main_to, 0, k)

                @pl.when(has_other)
                def _():
                    arrive(from_other, b, other_to, 1, k - 1)

                @pl.when(k < other_hops)
                def _():
                    send(from_other, b, other_to, 1, k)

                send(from_main, b, sibling, 2, k)

                @pl.when(has_other)
                def _():
                    send(from_other, b, sibling, 2, main_hops + k)

                if use is None:
                    continue

                def turn(q, inner):
                    live = jnp.logical_or(q % 2 == 0, has_other)

                    @pl.when(live)
                    def _():
                        there = jnp.where(
                            jnp.logical_or(q == 0, q == 3), from_main // 2, from_other // 2
                        )
                        source = there * 2 + jnp.where(q < 2, c, 1 - c)

                        @pl.when(q >= 2)
                        def _():
                            arrive(source, b, sibling, 2, k + jnp.where(q == 3, main_hops, 0))

                        use(source, b)

                    return inner

                lax.fori_loop(0, 4, turn, 0)
            return carry

        lax.fori_loop(0, main_hops + 1, step, 0)

        for k in range(main_hops):
            for b in range(2):
                sent(r, b, main_to, 0, k)
        for k in range(other_hops):
            for b in range(2):
                sent(r, b, other_to, 1, k)
        for k in range(main_hops + 1 + other_hops):
            for b in range(2):
                sent(r, b, sibling, 2, k)
                if use is None:
                    arrive(r, b, sibling, 2, k)

    rows_at = lax.broadcasted_iota(I32, (8, 128), 0)
    hot_first = n_row * slots + r * block
    cold_first = r * slots
    low = block // 8
    cold_low = slots // 8
    groups = low // 16

    def count(source, b):
        def tile(t, carry):
            first = pl.multiple_of(t * 128, 128)
            high, field = [], []
            for j in range(16):
                word = jnp.broadcast_to(notes[source, j : j + 1, pl.ds(first, 128)], (8, 128))
                value = word & 0xFFFF if b == 0 else lax.shift_right_logical(word, 16)
                hot = value - hot_first
                cold = value - cold_first
                is_hot = jnp.logical_and(hot >= 0, hot < block)
                is_cold = jnp.logical_and(cold >= 0, cold < slots)
                top = jnp.where(is_cold, cold // cold_low, lax.shift_right_logical(hot, low.bit_length() - 1) & 7)
                high.append(
                    jnp.where(is_cold, low + (cold & (cold_low - 1)), hot & (low - 1)) - rows_at
                )
                field.append(
                    jnp.where(
                        jnp.logical_or(is_hot, is_cold),
                        lax.shift_left(jnp.ones_like(top), (top & 7) * 4),
                        0,
                    )
                )
            for k in range(groups + 1):
                parts = []
                for h in range(2):
                    base = (k * 2 + h) * 8
                    sums = []
                    for g in range(2):
                        total = jnp.zeros((8, 128), I32)
                        for j in range(8 * g, 8 * g + 8):
                            total = total + jnp.where(high[j] == base, field[j], 0)
                        sums.append(total)
                    even = (sums[0] & NIBBLES) + (sums[1] & NIBBLES)
                    odd = (lax.shift_right_logical(sums[0], 4) & NIBBLES) + (
                        lax.shift_right_logical(sums[1], 4) & NIBBLES
                    )
                    parts.append((even, odd))
                for f in range(8):
                    found = []
                    for h in range(2):
                        x = lax.shift_right_logical(parts[h][f & 1], 8 * (f >> 1))
                        found.append((x & 255).astype(F32))
                    row = f * low + k * 16 if k < groups else block + f * 16
                    tally[pl.ds(row, 16), pl.ds(first, 128)] = jnp.concatenate(found, 0).astype(BF16)
            return carry

        lax.fori_loop(0, half // 128, tile, 0)
        rows = pools[source, pl.ds(b * half, half), :]
        hot_sum[...] += jnp.dot(tally[:block, :], rows, preferred_element_type=F32)
        cold = jnp.dot(tally[block:, :], rows, preferred_element_type=F32)
        if b == 0:
            cold_out[source] = cold
        else:
            cold_out[source] += cold
            cold_in[d, source] = cold_out[source, pl.ds(pl.multiple_of(d * CAP, CAP), CAP), :]
            held = notes[source, :, half:]
            wanted = lax.broadcasted_iota(I32, held.shape, 0) == r
            ids_out[source] = jnp.sum(jnp.where(wanted, held, 0), axis=0)

            def give(i, carry):
                to = peer(i)
                pltpu.make_async_remote_copy(
                    src_ref=cold_out.at[source, pl.ds(pl.multiple_of(to * CAP, CAP), CAP)],
                    dst_ref=cold_in.at[d, source],
                    send_sem=bulk_sems.at[0],
                    recv_sem=bulk_sems.at[1],
                    device_id=(to, r),
                    device_id_type=MESH,
                ).start()
                return carry

            lax.fori_loop(1, n_dp, give, 0)

    ring(pools, notes, pool_sems, note_sems, count)

    def to_all(make):
        def go(i, carry):
            make(peer(i)).start()
            return carry

        lax.fori_loop(1, n_dp, go, 0)

    def to_dp(src, dst, n):
        def make(to):
            return pltpu.make_async_remote_copy(
                src_ref=src(to),
                dst_ref=dst,
                send_sem=bulk_sems.at[n],
                recv_sem=bulk_sems.at[n + 1],
                device_id=(to, r),
                device_id_type=MESH,
            )

        return make

    def all_bytes(ref, n):
        return pltpu.make_async_remote_copy(
            src_ref=ref,
            dst_ref=ref,
            send_sem=bulk_sems.at[n],
            recv_sem=bulk_sems.at[n + 1],
            device_id=(peer(1), r),
            device_id_type=MESH,
        )

    others = pl.ds(0, n_dp - 1)
    to_all(
        to_dp(
            lambda to: hot_sum.at[pl.ds(pl.multiple_of(to * piece, piece), piece)], hot_in.at[d], 2
        )
    )
    ids_in[d] = ids_out[...]
    to_all(to_dp(lambda to: ids_out, ids_in.at[d], 4))
    mine = pl.ds(pl.multiple_of(d * piece, piece), piece)
    hot_in[d] = hot_sum[mine, :]
    all_bytes(hot_in.at[others], 2).wait_recv()
    grad = hot_in[0]
    for k in range(1, n_dp):
        grad = grad + hot_in[k]
    per_line = 128 // piece
    line_at = pl.ds(d // per_line, 1)
    first = lax.rem(d, per_line) * piece
    update, new_m, new_s, new_scale_m, new_scale_s = adam_parts(
        codes_m_ref[mine, :],
        codes_s_ref[mine, :],
        lanes_to_column(scale_m_ref[line_at, :], piece, first),
        lanes_to_column(scale_s_ref[line_at, :], piece, first),
        grad,
    )
    widest = jnp.maximum(jnp.max(jnp.abs(update), axis=1, keepdims=True), 1e-20)
    steps_q[r, mine, :] = jnp.round(update * (32767.0 / widest)).astype(I32).astype(jnp.int16)
    line_out[0:1, :] = column_to_lanes(new_scale_m, 128)
    line_out[1:2, :] = column_to_lanes(new_scale_s, 128)
    line_out[2:3, :] = column_to_lanes(widest / 32767.0, 128)
    line_out[3:8, :] = jnp.zeros((5, 128), F32)
    new_m_ref[mine, :] = new_m
    new_s_ref[mine, :] = new_s
    lines_ref[d] = line_out[...]
    to_all(to_dp(lambda to: line_out, lines_ref.at[d], 6))
    to_all(to_dp(lambda to: steps_q.at[r, mine], steps_q.at[r, mine], 8))
    to_all(to_dp(lambda to: new_m_ref.at[mine], new_m_ref.at[mine], 10))
    to_all(to_dp(lambda to: new_s_ref.at[mine], new_s_ref.at[mine], 12))
    all_bytes(lines_ref.at[others], 6).wait_recv()
    for k in range(n_dp):
        steps_scale[r, k : k + 1, :] = lines_ref[k, 2:3, :]
    rest = pl.ds(0, block - piece)
    all_bytes(steps_q.at[r, rest], 8).wait_recv()

    ring(steps_q, steps_scale, step_sems, step_scale_sems, None)

    for ref, n in (
        (cold_in.at[others], 0),
        (ids_in.at[others], 4),
        (new_m_ref.at[rest], 10),
        (new_s_ref.at[rest], 12),
    ):
        all_bytes(ref, n).wait()
    for ref, n in (
        (hot_in.at[others], 2),
        (lines_ref.at[others], 6),
        (steps_q.at[r, rest], 8),
    ):
        all_bytes(ref, n).wait_send()


def cold_kernel(
    values_ref,
    ids_ref,
    table_ref,
    codes_m_ref,
    codes_s_ref,
    scale_m_ref,
    scale_s_ref,
    table_out,
    codes_m_out,
    codes_s_out,
    scale_m_out,
    scale_s_out,
    split,
):
    n = pl.program_id(0)
    rows, width = table_ref.shape

    @pl.when(n == 0)
    def _():
        value = values_ref[...]
        top = value.astype(BF16)
        split[:, :width] = top
        split[:, width:] = (value - top.astype(F32)).astype(BF16)

    ids = ids_ref[...]
    shape = (rows, ids.shape[1])
    wanted = lax.broadcasted_iota(I32, shape, 0) + n * rows
    match = jnp.where(wanted == jnp.broadcast_to(ids, shape), 1.0, 0.0).astype(BF16)
    both = jnp.dot(match, split[...], preferred_element_type=F32)
    grad = both[:, :width] + both[:, width:]
    for k in range(rows // 128):
        at = slice(k * 128, (k + 1) * 128)
        line = pl.ds(n * (rows // 128) + k, 1)
        update, new_m, new_s, scale_m, scale_s = adam_parts(
            codes_m_ref[at, :],
            codes_s_ref[at, :],
            lanes_to_column(scale_m_ref[line, :], 128, 0),
            lanes_to_column(scale_s_ref[line, :], 128, 0),
            grad[at, :],
        )
        table_out[at, :] = table_ref[at, :] - update
        codes_m_out[at, :] = new_m
        codes_s_out[at, :] = new_s
        scale_m_out[line, :] = column_to_lanes(scale_m, 128)
        scale_s_out[line, :] = column_to_lanes(scale_s, 128)


def replica_kernel(table_ref, steps_ref, scale_ref, out_ref):
    piece = table_ref.shape[0] // scale_ref.shape[1]
    for k in range(scale_ref.shape[1]):
        at = slice(k * piece, (k + 1) * piece)
        scale = lanes_to_column(scale_ref[0, k : k + 1, :], piece, 0)
        out_ref[at, :] = table_ref[at, :] - steps_ref[0, at, :].astype(I32).astype(F32) * scale


def body(
    n_dp,
    n_row,
    bag_index,
    pooled_grad,
    touched_ids,
    owner_counts,
    cold_table,
    cold_moment_codes,
    cold_second_codes,
    cold_moment_scales,
    cold_second_scales,
    hot_table,
    hot_moment_codes,
    hot_second_codes,
    hot_moment_scales,
    hot_second_scales,
):
    samples, pool = bag_index.shape
    touch_rows = touched_ids.shape[1]
    width = pooled_grad.shape[1]
    hot_rows = hot_table.shape[0]
    own_rows = cold_table.shape[0]
    block = hot_rows // n_row
    slots = n_dp * CAP
    owners = n_dp * n_row

    counts = owner_counts[0]
    ends = jnp.cumsum(counts)
    spare = CAP - counts
    bag = bag_index.T
    padding = jnp.sum(
        jnp.where(ends[:, None, None] <= bag[None], spare[:, None, None], 0), axis=0
    )
    spread = bag + padding
    owner, place = spread // CAP, spread % CAP
    slot = (owner % n_row) * slots + (owner // n_row) * CAP + place
    code = jnp.where(bag < touch_rows, slot, bag - touch_rows + owners * CAP)
    packed = code[:, : samples // 2] | (code[:, samples // 2 :] << 16)
    lane = lax.broadcasted_iota(I32, (n_row, n_dp, CAP), 2)
    by_row = counts.reshape(n_dp, n_row).T
    starts = (ends - counts).reshape(n_dp, n_row).T
    position = jnp.where(lane < by_row[:, :, None], starts[:, :, None] + lane, -1).reshape(n_row, slots)
    spots = lax.iota(I32, touch_rows)
    slot_ids = jnp.sum(
        jnp.where(spots[:, None, None] == position[None], touched_ids[0][:, None, None] + 1, 0), axis=0
    ) - 1
    note = jnp.concatenate([packed, slot_ids], axis=1)

    chips = n_row // 2
    main_hops, other_hops = chips // 2, chips // 2 - 1
    flows = main_hops + 1 + other_hops
    vmem = pl.BlockSpec(memory_space=pltpu.VMEM)
    cold_in, ids_in, steps_q, steps_scale, new_m, new_s, lines = pl.pallas_call(
        functools.partial(exchange_kernel, n_dp, n_row),
        out_shape=(
            jax.ShapeDtypeStruct((n_dp, n_row, CAP, width), F32),
            jax.ShapeDtypeStruct((n_dp, n_row, slots), I32),
            jax.ShapeDtypeStruct((n_row, block, width), jnp.int16),
            jax.ShapeDtypeStruct((n_row, n_dp, 128), F32),
            jax.ShapeDtypeStruct((block, width), BF16),
            jax.ShapeDtypeStruct((block, width), BF16),
            jax.ShapeDtypeStruct((n_dp, 8, 128), F32),
        ),
        in_specs=[vmem] * 6,
        out_specs=(vmem,) * 7,
        scratch_shapes=[
            pltpu.VMEM((n_row, samples, width), BF16),
            pltpu.VMEM((n_row, pool, samples // 2 + slots), I32),
            pltpu.VMEM((block + slots, samples // 2), BF16),
            pltpu.VMEM((block, width), F32),
            pltpu.VMEM((n_row, slots, width), F32),
            pltpu.VMEM((n_row, slots), I32),
            pltpu.VMEM((n_dp, block // n_dp, width), F32),
            pltpu.VMEM((8, 128), F32),
            pltpu.SemaphoreType.DMA((6, 2 * flows)),
            pltpu.SemaphoreType.DMA((6, flows)),
            pltpu.SemaphoreType.DMA((6, 2 * flows)),
            pltpu.SemaphoreType.DMA((6, flows)),
            pltpu.SemaphoreType.DMA((14,)),
            pltpu.SemaphoreType.DMA((2,)),
        ],
        compiler_params=pltpu.CompilerParams(
            collective_id=0, has_side_effects=True, vmem_limit_bytes=48 * 1024 * 1024
        ),
    )(
        pooled_grad,
        note,
        hot_moment_codes,
        hot_second_codes,
        hot_moment_scales.reshape(-1, 128),
        hot_second_scales.reshape(-1, 128),
    )

    ids = lax.dynamic_slice_in_dim(ids_in, lax.axis_index("dp") * CAP, CAP, 2).reshape(1, -1)
    tile = own_rows // 4
    lines_of = own_rows // 128
    whole = lambda a, b: pl.BlockSpec((a, b), lambda n: (0, 0))
    rows = pl.BlockSpec((tile, width), lambda n: (n, 0))
    cold = pl.pallas_call(
        cold_kernel,
        grid=(own_rows // tile,),
        out_shape=(
            jax.ShapeDtypeStruct((own_rows, width), F32),
            jax.ShapeDtypeStruct((own_rows, width), BF16),
            jax.ShapeDtypeStruct((own_rows, width), BF16),
            jax.ShapeDtypeStruct((lines_of, 128), F32),
            jax.ShapeDtypeStruct((lines_of, 128), F32),
        ),
        in_specs=[
            whole(owners * CAP, width),
            whole(1, owners * CAP),
            rows,
            rows,
            rows,
            whole(lines_of, 128),
            whole(lines_of, 128),
        ],
        out_specs=(rows, rows, rows, whole(lines_of, 128), whole(lines_of, 128)),
        scratch_shapes=[pltpu.VMEM((owners * CAP, 2 * width), BF16)],
    )(
        cold_in.reshape(-1, width),
        ids,
        cold_table,
        cold_moment_codes,
        cold_second_codes,
        cold_moment_scales.reshape(-1, 128),
        cold_second_scales.reshape(-1, 128),
    )
    replica = pl.pallas_call(
        replica_kernel,
        grid=(n_row,),
        out_shape=jax.ShapeDtypeStruct((hot_rows, width), F32),
        in_specs=[
            pl.BlockSpec((block, width), lambda n: (n, 0)),
            pl.BlockSpec((1, block, width), lambda n: (n, 0, 0)),
            pl.BlockSpec((1, n_dp, 128), lambda n: (n, 0, 0)),
        ],
        out_specs=pl.BlockSpec((block, width), lambda n: (n, 0)),
    )(hot_table, steps_q, steps_scale)
    piece = block // n_dp
    return (
        cold[0],
        cold[1],
        cold[2],
        cold[3].reshape(-1),
        cold[4].reshape(-1),
        replica,
        new_m,
        new_s,
        lines[:, 0, :piece].reshape(-1),
        lines[:, 1, :piece].reshape(-1),
    )


def solution(mesh):
    both = P(("dp", "row"), None)
    line = P(("dp", "row"))
    return jax.shard_map(
        functools.partial(body, mesh.shape["dp"], mesh.shape["row"]),
        mesh=mesh,
        in_specs=(
            both,
            both,
            both,
            both,
            both,
            both,
            both,
            line,
            line,
            P(),
            P("row", None),
            P("row", None),
            P("row"),
            P("row"),
        ),
        out_specs=(
            both,
            both,
            both,
            line,
            line,
            P(),
            P("row", None),
            P("row", None),
            P("row"),
            P("row"),
        ),
        check_vma=False,
    )
```

```python
import functools

import jax
import jax.numpy as jnp
from jax import lax
from jax.experimental import pallas as pl
from jax.experimental.pallas import tpu as pltpu
from jax.sharding import PartitionSpec as P

CAP = 8
beta_one = 0.9
beta_two = 0.999
learn_rate = 0.1
adam_eps = 1e-08
bias_one = 1.0 - 1.7478712517226947e-46
bias_two = 0.6323045752290363

MESH = pl.DeviceIdType.MESH
F32 = jnp.float32
BF16 = jnp.bfloat16
I32 = jnp.int32
NIBBLES = 0x0F0F0F0F


def adam_parts(codes_m, codes_s, scale_m, scale_s, grad):
    moment = beta_one * scale_m * codes_m.astype(F32) + (1.0 - beta_one) * grad
    second = beta_two * scale_s * codes_s.astype(F32) + (1.0 - beta_two) * grad * grad
    update = learn_rate * (moment / bias_one) / (jnp.sqrt(second / bias_two) + adam_eps)
    new_m = jnp.max(jnp.abs(moment), axis=1, keepdims=True) + 1e-06
    new_s = jnp.max(second, axis=1, keepdims=True) + 1e-06
    return (
        update,
        (moment / new_m).astype(BF16),
        (second / new_s).astype(BF16),
        new_m,
        new_s,
    )


def lanes_to_column(line, rows, first):
    shape = (rows, line.shape[1])
    at = lax.broadcasted_iota(I32, shape, 1) == lax.broadcasted_iota(I32, shape, 0) + first
    return jnp.sum(jnp.where(at, jnp.broadcast_to(line, shape), 0.0), axis=1, keepdims=True)


def column_to_lanes(column, lanes):
    shape = (column.shape[0], lanes)
    at = lax.broadcasted_iota(I32, shape, 1) == lax.broadcasted_iota(I32, shape, 0)
    return jnp.sum(jnp.where(at, jnp.broadcast_to(column, shape), 0.0), axis=0, keepdims=True)


def note_kernel(n_dp, n_row, counts_ref, touched_ref, bag, note_ref):
    slots = n_dp * CAP
    half = bag.shape[1] // 2
    lane = lax.broadcasted_iota(I32, (n_row, slots), 1)
    owner_of = (lane // CAP) * n_row + lax.broadcasted_iota(I32, (n_row, slots), 0)
    entries = bag[...]

    def owner_step(o, carry):
        padding, start_of, count_of, start = carry
        held = counts_ref[0, o]
        end = start + held
        here = owner_of == o
        return (
            padding + jnp.where(entries >= end, CAP - held, 0),
            jnp.where(here, start, start_of),
            jnp.where(here, held, count_of),
            end,
        )

    none = jnp.zeros((n_row, slots), I32)
    padding, start_of, count_of, _ = lax.fori_loop(
        0, n_dp * n_row, owner_step, (jnp.zeros_like(entries), none, none, jnp.int32(0)), unroll=8
    )
    spread = entries + padding
    owner, place = spread // CAP, spread & (CAP - 1)
    slot = (owner & (n_row - 1)) * slots + (owner // n_row) * CAP + place
    touch_rows = touched_ref.shape[1]
    code = jnp.where(entries < touch_rows, slot, entries - touch_rows + n_row * slots)
    note_ref[:, :half] = code[:, :half] | lax.shift_left(code[:, half:], 16)
    position = jnp.where((lane & (CAP - 1)) < count_of, start_of + (lane & (CAP - 1)), -1)

    def touched_step(t, found):
        return jnp.where(position == t, touched_ref[0, t], found)

    note_ref[:, half:] = lax.fori_loop(0, touch_rows, touched_step, none - 1, unroll=16)


def exchange_kernel(
    n_dp,
    n_row,
    pool_ref,
    note_ref,
    codes_m_ref,
    codes_s_ref,
    scale_m_ref,
    scale_s_ref,
    cold_in,
    ids_in,
    steps_q,
    steps_scale,
    new_m_ref,
    new_s_ref,
    lines_ref,
    pools,
    notes,
    tally,
    hot_sum,
    cold_out,
    ids_out,
    hot_in,
    line_out,
    pool_sems,
    note_sems,
    step_sems,
    step_scale_sems,
    bulk_sems,
    local_sems,
):
    d = lax.axis_index("dp")
    r = lax.axis_index("row")
    chips = n_row // 2
    z, c = r // 2, r % 2
    sign = 1 - 2 * c
    half = pool_ref.shape[0] // 2
    block = hot_sum.shape[0]
    piece = block // n_dp
    slots = n_dp * CAP
    main_hops, other_hops = chips // 2, chips // 2 - 1

    def row_of(chip, core):
        return lax.rem(chip + 2 * chips, chips) * 2 + core

    main_to = row_of(z + sign, c)
    other_to = row_of(z - sign, c)
    sibling = row_of(z, 1 - c)

    def peer(i):
        return lax.rem(d + i, n_dp)

    own = pltpu.make_async_copy(pool_ref, pools.at[r], local_sems.at[0])
    own_note = pltpu.make_async_copy(note_ref, notes.at[r], local_sems.at[1])
    own.start()
    own_note.start()

    barrier = pltpu.get_barrier_semaphore()
    for to in (main_to, other_to, sibling):
        pl.semaphore_signal(barrier, inc=1, device_id=(d, to), device_id_type=MESH)

    def greet(i, carry):
        pl.semaphore_signal(barrier, inc=1, device_id=(peer(i), r), device_id_type=MESH)
        return carry

    lax.fori_loop(1, n_dp, greet, 0)
    own.wait()
    own_note.wait()
    hot_sum[...] = jnp.zeros_like(hot_sum)
    pl.semaphore_wait(barrier, n_dp + 2)

    def ring(big, small, big_sems, small_sems, use):
        span = big.shape[1] // 2

        def copies(source, b, to, lane, k):
            at = big.at[source, pl.ds(b * span, span)]
            n = k * 2 + b
            yield pltpu.make_async_remote_copy(
                src_ref=at,
                dst_ref=at,
                send_sem=big_sems.at[2 * lane, n],
                recv_sem=big_sems.at[2 * lane + 1, n],
                device_id=(d, to),
                device_id_type=MESH,
            )

        def note(source, to, lane, k):
            return pltpu.make_async_remote_copy(
                src_ref=small.at[source],
                dst_ref=small.at[source],
                send_sem=small_sems.at[2 * lane, k],
                recv_sem=small_sems.at[2 * lane + 1, k],
                device_id=(d, to),
                device_id_type=MESH,
            )

        def send(source, b, to, lane, k):
            if b == 0:
                note(source, to, lane, k).start()
            for copy in copies(source, b, to, lane, k):
                copy.start()

        def arrive(source, b, to, lane, k):
            if b == 0:
                note(source, to, lane, k).wait_recv()
            for copy in copies(source, b, to, lane, k):
                copy.wait_recv()

        def sent(source, b, to, lane, k):
            if b == 0:
                note(source, to, lane, k).wait_send()
            for copy in copies(source, b, to, lane, k):
                copy.wait_send()

        def step(k, carry):
            from_main = row_of(z - sign * k, c)
            from_other = row_of(z + sign * k, c)
            has_other = jnp.logical_and(k >= 1, k <= other_hops)
            for b in range(2):

                @pl.when(k >= 1)
                def _():
                    arrive(from_main, b, main_to, 0, k - 1)

                @pl.when(k < main_hops)
                def _():
                    send(from_main, b, main_to, 0, k)

                @pl.when(has_other)
                def _():
                    arrive(from_other, b, other_to, 1, k - 1)

                @pl.when(k < other_hops)
                def _():
                    send(from_other, b, other_to, 1, k)

                send(from_main, b, sibling, 2, k)

                @pl.when(has_other)
                def _():
                    send(from_other, b, sibling, 2, main_hops + k)

                if use is None:
                    continue

                def turn(q, inner):
                    live = jnp.logical_or(q % 2 == 0, has_other)

                    @pl.when(live)
                    def _():
                        there = jnp.where(
                            jnp.logical_or(q == 0, q == 3), from_main // 2, from_other // 2
                        )
                        source = there * 2 + jnp.where(q < 2, c, 1 - c)

                        @pl.when(q >= 2)
                        def _():
                            arrive(source, b, sibling, 2, k + jnp.where(q == 3, main_hops, 0))

                        use(source, b)

                    return inner

                lax.fori_loop(0, 4, turn, 0)
            return carry

        lax.fori_loop(0, main_hops + 1, step, 0)

        for k in range(main_hops):
            for b in range(2):
                sent(r, b, main_to, 0, k)
        for k in range(other_hops):
            for b in range(2):
                sent(r, b, other_to, 1, k)
        for k in range(main_hops + 1 + other_hops):
            for b in range(2):
                sent(r, b, sibling, 2, k)
                if use is None:
                    arrive(r, b, sibling, 2, k)

    rows_at = lax.broadcasted_iota(I32, (8, 128), 0)
    hot_first = n_row * slots + r * block
    cold_first = r * slots
    low = block // 8
    cold_low = slots // 8
    groups = low // 16

    def count(source, b):
        def tile(t, carry):
            first = pl.multiple_of(t * 128, 128)
            high, field = [], []
            for j in range(16):
                word = jnp.broadcast_to(notes[source, j : j + 1, pl.ds(first, 128)], (8, 128))
                value = word & 0xFFFF if b == 0 else lax.shift_right_logical(word, 16)
                hot = value - hot_first
                cold = value - cold_first
                is_hot = jnp.logical_and(hot >= 0, hot < block)
                is_cold = jnp.logical_and(cold >= 0, cold < slots)
                top = jnp.where(is_cold, cold // cold_low, lax.shift_right_logical(hot, low.bit_length() - 1) & 7)
                high.append(
                    jnp.where(is_cold, low + (cold & (cold_low - 1)), hot & (low - 1)) - rows_at
                )
                field.append(
                    jnp.where(
                        jnp.logical_or(is_hot, is_cold),
                        lax.shift_left(jnp.ones_like(top), (top & 7) * 4),
                        0,
                    )
                )
            for k in range(groups + 1):
                parts = []
                for h in range(2):
                    base = (k * 2 + h) * 8
                    sums = []
                    for g in range(2):
                        total = jnp.zeros((8, 128), I32)
                        for j in range(8 * g, 8 * g + 8):
                            total = total + jnp.where(high[j] == base, field[j], 0)
                        sums.append(total)
                    even = (sums[0] & NIBBLES) + (sums[1] & NIBBLES)
                    odd = (lax.shift_right_logical(sums[0], 4) & NIBBLES) + (
                        lax.shift_right_logical(sums[1], 4) & NIBBLES
                    )
                    parts.append((even, odd))
                for f in range(8):
                    found = []
                    for h in range(2):
                        x = lax.shift_right_logical(parts[h][f & 1], 8 * (f >> 1))
                        found.append((x & 255).astype(F32))
                    row = f * low + k * 16 if k < groups else block + f * 16
                    tally[pl.ds(row, 16), pl.ds(first, 128)] = jnp.concatenate(found, 0).astype(BF16)
            return carry

        lax.fori_loop(0, half // 128, tile, 0)
        rows = pools[source, pl.ds(b * half, half), :]
        hot_sum[...] += jnp.dot(tally[:block, :], rows, preferred_element_type=F32)
        cold = jnp.dot(tally[block:, :], rows, preferred_element_type=F32)
        if b == 0:
            cold_out[source] = cold
        else:
            cold_out[source] += cold
            cold_in[d, source] = cold_out[source, pl.ds(pl.multiple_of(d * CAP, CAP), CAP), :]
            held = notes[source, :, half:]
            wanted = lax.broadcasted_iota(I32, held.shape, 0) == r
            ids_out[source] = jnp.sum(jnp.where(wanted, held, 0), axis=0)

            def give(i, carry):
                to = peer(i)
                pltpu.make_async_remote_copy(
                    src_ref=cold_out.at[source, pl.ds(pl.multiple_of(to * CAP, CAP), CAP)],
                    dst_ref=cold_in.at[d, source],
                    send_sem=bulk_sems.at[0],
                    recv_sem=bulk_sems.at[1],
                    device_id=(to, r),
                    device_id_type=MESH,
                ).start()
                return carry

            lax.fori_loop(1, n_dp, give, 0)

    ring(pools, notes, pool_sems, note_sems, count)

    def to_all(make):
        def go(i, carry):
            make(peer(i)).start()
            return carry

        lax.fori_loop(1, n_dp, go, 0)

    def to_dp(src, dst, n):
        def make(to):
            return pltpu.make_async_remote_copy(
                src_ref=src(to),
                dst_ref=dst,
                send_sem=bulk_sems.at[n],
                recv_sem=bulk_sems.at[n + 1],
                device_id=(to, r),
                device_id_type=MESH,
            )

        return make

    def all_bytes(ref, n):
        return pltpu.make_async_remote_copy(
            src_ref=ref,
            dst_ref=ref,
            send_sem=bulk_sems.at[n],
            recv_sem=bulk_sems.at[n + 1],
            device_id=(peer(1), r),
            device_id_type=MESH,
        )

    others = pl.ds(0, n_dp - 1)
    to_all(
        to_dp(
            lambda to: hot_sum.at[pl.ds(pl.multiple_of(to * piece, piece), piece)], hot_in.at[d], 2
        )
    )
    ids_in[d] = ids_out[...]
    to_all(to_dp(lambda to: ids_out, ids_in.at[d], 4))
    mine = pl.ds(pl.multiple_of(d * piece, piece), piece)
    hot_in[d] = hot_sum[mine, :]
    all_bytes(hot_in.at[others], 2).wait_recv()
    grad = hot_in[0]
    for k in range(1, n_dp):
        grad = grad + hot_in[k]
    per_line = 128 // piece
    line_at = pl.ds(d // per_line, 1)
    first = lax.rem(d, per_line) * piece
    update, new_m, new_s, new_scale_m, new_scale_s = adam_parts(
        codes_m_ref[mine, :],
        codes_s_ref[mine, :],
        lanes_to_column(scale_m_ref[line_at, :], piece, first),
        lanes_to_column(scale_s_ref[line_at, :], piece, first),
        grad,
    )
    widest = jnp.maximum(jnp.max(jnp.abs(update), axis=1, keepdims=True), 1e-20)
    steps_q[r, mine, :] = jnp.round(update * (32767.0 / widest)).astype(I32).astype(jnp.int16)
    line_out[0:1, :] = column_to_lanes(new_scale_m, 128)
    line_out[1:2, :] = column_to_lanes(new_scale_s, 128)
    line_out[2:3, :] = column_to_lanes(widest / 32767.0, 128)
    line_out[3:8, :] = jnp.zeros((5, 128), F32)
    new_m_ref[mine, :] = new_m
    new_s_ref[mine, :] = new_s
    lines_ref[d] = line_out[...]
    to_all(to_dp(lambda to: line_out, lines_ref.at[d], 6))
    to_all(to_dp(lambda to: steps_q.at[r, mine], steps_q.at[r, mine], 8))
    to_all(to_dp(lambda to: new_m_ref.at[mine], new_m_ref.at[mine], 10))
    to_all(to_dp(lambda to: new_s_ref.at[mine], new_s_ref.at[mine], 12))
    all_bytes(lines_ref.at[others], 6).wait_recv()
    for k in range(n_dp):
        steps_scale[r, k : k + 1, :] = lines_ref[k, 2:3, :]
    rest = pl.ds(0, block - piece)
    all_bytes(steps_q.at[r, rest], 8).wait_recv()

    ring(steps_q, steps_scale, step_sems, step_scale_sems, None)

    for ref, n in (
        (cold_in.at[others], 0),
        (ids_in.at[others], 4),
        (new_m_ref.at[rest], 10),
        (new_s_ref.at[rest], 12),
    ):
        all_bytes(ref, n).wait()
    for ref, n in (
        (hot_in.at[others], 2),
        (lines_ref.at[others], 6),
        (steps_q.at[r, rest], 8),
    ):
        all_bytes(ref, n).wait_send()


def cold_kernel(
    values_ref,
    ids_ref,
    table_ref,
    codes_m_ref,
    codes_s_ref,
    scale_m_ref,
    scale_s_ref,
    table_out,
    codes_m_out,
    codes_s_out,
    scale_m_out,
    scale_s_out,
    split,
):
    n = pl.program_id(0)
    rows, width = table_ref.shape

    @pl.when(n == 0)
    def _():
        value = values_ref[...]
        top = value.astype(BF16)
        split[:, :width] = top
        split[:, width:] = (value - top.astype(F32)).astype(BF16)

    ids = ids_ref[...]
    shape = (rows, ids.shape[1])
    wanted = lax.broadcasted_iota(I32, shape, 0) + n * rows
    match = jnp.where(wanted == jnp.broadcast_to(ids, shape), 1.0, 0.0).astype(BF16)
    both = jnp.dot(match, split[...], preferred_element_type=F32)
    grad = both[:, :width] + both[:, width:]
    for k in range(rows // 128):
        at = slice(k * 128, (k + 1) * 128)
        line = pl.ds(n * (rows // 128) + k, 1)
        update, new_m, new_s, scale_m, scale_s = adam_parts(
            codes_m_ref[at, :],
            codes_s_ref[at, :],
            lanes_to_column(scale_m_ref[line, :], 128, 0),
            lanes_to_column(scale_s_ref[line, :], 128, 0),
            grad[at, :],
        )
        table_out[at, :] = table_ref[at, :] - update
        codes_m_out[at, :] = new_m
        codes_s_out[at, :] = new_s
        scale_m_out[line, :] = column_to_lanes(scale_m, 128)
        scale_s_out[line, :] = column_to_lanes(scale_s, 128)


def replica_kernel(table_ref, steps_ref, scale_ref, out_ref):
    blocks, pieces = scale_ref.shape[:2]
    block = steps_ref.shape[1]
    piece = block // pieces
    for n in range(blocks):
        for k in range(pieces):
            at = slice(n * block + k * piece, n * block + (k + 1) * piece)
            scale = lanes_to_column(scale_ref[n, k : k + 1, :], piece, 0)
            moved = steps_ref[n, k * piece : (k + 1) * piece, :].astype(I32).astype(F32)
            out_ref[at, :] = table_ref[at, :] - moved * scale


def body(
    n_dp,
    n_row,
    bag_index,
    pooled_grad,
    touched_ids,
    owner_counts,
    cold_table,
    cold_moment_codes,
    cold_second_codes,
    cold_moment_scales,
    cold_second_scales,
    hot_table,
    hot_moment_codes,
    hot_second_codes,
    hot_moment_scales,
    hot_second_scales,
):
    samples, pool = bag_index.shape
    width = pooled_grad.shape[1]
    hot_rows = hot_table.shape[0]
    own_rows = cold_table.shape[0]
    block = hot_rows // n_row
    slots = n_dp * CAP
    owners = n_dp * n_row

    vmem = pl.BlockSpec(memory_space=pltpu.VMEM)
    smem = pl.BlockSpec(memory_space=pltpu.SMEM)
    note = pl.pallas_call(
        functools.partial(note_kernel, n_dp, n_row),
        out_shape=jax.ShapeDtypeStruct((pool, samples // 2 + slots), I32),
        in_specs=[smem, smem, vmem],
        out_specs=vmem,
        compiler_params=pltpu.CompilerParams(vmem_limit_bytes=63 * 1024 * 1024),
    )(owner_counts, touched_ids, bag_index.T)

    chips = n_row // 2
    main_hops, other_hops = chips // 2, chips // 2 - 1
    flows = main_hops + 1 + other_hops
    cold_in, ids_in, steps_q, steps_scale, new_m, new_s, lines = pl.pallas_call(
        functools.partial(exchange_kernel, n_dp, n_row),
        out_shape=(
            jax.ShapeDtypeStruct((n_dp, n_row, CAP, width), F32),
            jax.ShapeDtypeStruct((n_dp, n_row, slots), I32),
            jax.ShapeDtypeStruct((n_row, block, width), jnp.int16),
            jax.ShapeDtypeStruct((n_row, n_dp, 128), F32),
            jax.ShapeDtypeStruct((block, width), BF16),
            jax.ShapeDtypeStruct((block, width), BF16),
            jax.ShapeDtypeStruct((n_dp, 8, 128), F32),
        ),
        in_specs=[vmem] * 6,
        out_specs=(vmem,) * 7,
        scratch_shapes=[
            pltpu.VMEM((n_row, samples, width), BF16),
            pltpu.VMEM((n_row, pool, samples // 2 + slots), I32),
            pltpu.VMEM((block + slots, samples // 2), BF16),
            pltpu.VMEM((block, width), F32),
            pltpu.VMEM((n_row, slots, width), F32),
            pltpu.VMEM((n_row, slots), I32),
            pltpu.VMEM((n_dp, block // n_dp, width), F32),
            pltpu.VMEM((8, 128), F32),
            pltpu.SemaphoreType.DMA((6, 2 * flows)),
            pltpu.SemaphoreType.DMA((6, flows)),
            pltpu.SemaphoreType.DMA((6, 2 * flows)),
            pltpu.SemaphoreType.DMA((6, flows)),
            pltpu.SemaphoreType.DMA((14,)),
            pltpu.SemaphoreType.DMA((2,)),
        ],
        compiler_params=pltpu.CompilerParams(
            collective_id=0, has_side_effects=True, vmem_limit_bytes=63 * 1024 * 1024
        ),
    )(
        pooled_grad,
        note,
        hot_moment_codes,
        hot_second_codes,
        hot_moment_scales.reshape(-1, 128),
        hot_second_scales.reshape(-1, 128),
    )

    ids = lax.dynamic_slice_in_dim(ids_in, lax.axis_index("dp") * CAP, CAP, 2).reshape(1, -1)
    tile = own_rows // 4
    lines_of = own_rows // 128
    whole = lambda a, b: pl.BlockSpec((a, b), lambda n: (0, 0))
    rows = pl.BlockSpec((tile, width), lambda n: (n, 0))
    cold = pl.pallas_call(
        cold_kernel,
        grid=(own_rows // tile,),
        out_shape=(
            jax.ShapeDtypeStruct((own_rows, width), F32),
            jax.ShapeDtypeStruct((own_rows, width), BF16),
            jax.ShapeDtypeStruct((own_rows, width), BF16),
            jax.ShapeDtypeStruct((lines_of, 128), F32),
            jax.ShapeDtypeStruct((lines_of, 128), F32),
        ),
        in_specs=[
            whole(owners * CAP, width),
            whole(1, owners * CAP),
            rows,
            rows,
            rows,
            whole(lines_of, 128),
            whole(lines_of, 128),
        ],
        out_specs=(rows, rows, rows, whole(lines_of, 128), whole(lines_of, 128)),
        scratch_shapes=[pltpu.VMEM((owners * CAP, 2 * width), BF16)],
    )(
        cold_in.reshape(-1, width),
        ids,
        cold_table,
        cold_moment_codes,
        cold_second_codes,
        cold_moment_scales.reshape(-1, 128),
        cold_second_scales.reshape(-1, 128),
    )
    replica = pl.pallas_call(
        replica_kernel,
        grid=(n_row // 4,),
        out_shape=jax.ShapeDtypeStruct((hot_rows, width), F32),
        in_specs=[
            pl.BlockSpec((4 * block, width), lambda n: (n, 0)),
            pl.BlockSpec((4, block, width), lambda n: (n, 0, 0)),
            pl.BlockSpec((4, n_dp, 128), lambda n: (n, 0, 0)),
        ],
        out_specs=pl.BlockSpec((4 * block, width), lambda n: (n, 0)),
    )(hot_table, steps_q, steps_scale)
    piece = block // n_dp
    return (
        cold[0],
        cold[1],
        cold[2],
        cold[3].reshape(-1),
        cold[4].reshape(-1),
        replica,
        new_m,
        new_s,
        lines[:, 0, :piece].reshape(-1),
        lines[:, 1, :piece].reshape(-1),
    )


def solution(mesh):
    both = P(("dp", "row"), None)
    line = P(("dp", "row"))
    return jax.shard_map(
        functools.partial(body, mesh.shape["dp"], mesh.shape["row"]),
        mesh=mesh,
        in_specs=(
            both,
            both,
            both,
            both,
            both,
            both,
            both,
            line,
            line,
            P(),
            P("row", None),
            P("row", None),
            P("row"),
            P("row"),
        ),
        out_specs=(
            both,
            both,
            both,
            line,
            line,
            P(),
            P("row", None),
            P("row", None),
            P("row"),
            P("row"),
        ),
        check_vma=False,
    )
```

```python
import functools

import jax
import jax.numpy as jnp
from jax import lax
from jax.experimental import pallas as pl
from jax.experimental.pallas import tpu as pltpu
from jax.sharding import PartitionSpec as P

CAP = 8
beta_one = 0.9
beta_two = 0.999
learn_rate = 0.1
adam_eps = 1e-08
bias_one = 1.0 - 1.7478712517226947e-46
bias_two = 0.6323045752290363

MESH = pl.DeviceIdType.MESH
F32 = jnp.float32
BF16 = jnp.bfloat16
I32 = jnp.int32
NIBBLES = 0x0F0F0F0F


def adam_parts(codes_m, codes_s, scale_m, scale_s, grad):
    moment = beta_one * scale_m * codes_m.astype(F32) + (1.0 - beta_one) * grad
    second = beta_two * scale_s * codes_s.astype(F32) + (1.0 - beta_two) * grad * grad
    update = learn_rate * (moment / bias_one) / (jnp.sqrt(second / bias_two) + adam_eps)
    new_m = jnp.max(jnp.abs(moment), axis=1, keepdims=True) + 1e-06
    new_s = jnp.max(second, axis=1, keepdims=True) + 1e-06
    return (
        update,
        (moment / new_m).astype(BF16),
        (second / new_s).astype(BF16),
        new_m,
        new_s,
    )


def lanes_to_column(line, rows, first):
    shape = (rows, line.shape[1])
    at = lax.broadcasted_iota(I32, shape, 1) == lax.broadcasted_iota(I32, shape, 0) + first
    return jnp.sum(jnp.where(at, jnp.broadcast_to(line, shape), 0.0), axis=1, keepdims=True)


def column_to_lanes(column, lanes):
    shape = (column.shape[0], lanes)
    at = lax.broadcasted_iota(I32, shape, 1) == lax.broadcasted_iota(I32, shape, 0)
    return jnp.sum(jnp.where(at, jnp.broadcast_to(column, shape), 0.0), axis=0, keepdims=True)


def note_kernel(n_dp, n_row, counts_ref, touched_ref, bag, note_ref):
    slots = n_dp * CAP
    half = bag.shape[1] // 2
    lane = lax.broadcasted_iota(I32, (n_row, slots), 1)
    owner_of = (lane // CAP) * n_row + lax.broadcasted_iota(I32, (n_row, slots), 0)
    entries = bag[...]

    def owner_step(o, carry):
        padding, start_of, count_of, start = carry
        held = counts_ref[0, o]
        end = start + held
        here = owner_of == o
        return (
            padding + jnp.where(entries >= end, CAP - held, 0),
            jnp.where(here, start, start_of),
            jnp.where(here, held, count_of),
            end,
        )

    none = jnp.zeros((n_row, slots), I32)
    padding, start_of, count_of, _ = lax.fori_loop(
        0, n_dp * n_row, owner_step, (jnp.zeros_like(entries), none, none, jnp.int32(0)), unroll=8
    )
    spread = entries + padding
    owner, place = spread // CAP, spread & (CAP - 1)
    slot = (owner & (n_row - 1)) * slots + (owner // n_row) * CAP + place
    touch_rows = touched_ref.shape[1]
    code = jnp.where(entries < touch_rows, slot, entries - touch_rows + n_row * slots)
    note_ref[:, :half] = code[:, :half] | lax.shift_left(code[:, half:], 16)
    position = jnp.where((lane & (CAP - 1)) < count_of, start_of + (lane & (CAP - 1)), -1)

    def touched_step(t, found):
        return jnp.where(position == t, touched_ref[0, t], found)

    note_ref[:, half:] = lax.fori_loop(0, touch_rows, touched_step, none - 1, unroll=16)


def exchange_kernel(
    n_dp,
    n_row,
    pool_ref,
    note_ref,
    codes_m_ref,
    codes_s_ref,
    scale_m_ref,
    scale_s_ref,
    cold_in,
    ids_in,
    steps_q,
    steps_scale,
    new_m_ref,
    new_s_ref,
    lines_ref,
    pools,
    notes,
    tally,
    hot_sum,
    cold_out,
    ids_out,
    hot_in,
    line_out,
    pool_sems,
    note_sems,
    step_sems,
    step_scale_sems,
    bulk_sems,
    local_sems,
):
    d = lax.axis_index("dp")
    r = lax.axis_index("row")
    chips = n_row // 2
    z, c = r // 2, r % 2
    sign = 1 - 2 * c
    half = pool_ref.shape[0] // 2
    block = hot_sum.shape[0]
    piece = block // n_dp
    slots = n_dp * CAP
    main_hops, other_hops = chips // 2, chips // 2 - 1

    def row_of(chip, core):
        return lax.rem(chip + 2 * chips, chips) * 2 + core

    main_to = row_of(z + sign, c)
    other_to = row_of(z - sign, c)
    sibling = row_of(z, 1 - c)

    def peer(i):
        return lax.rem(d + i, n_dp)

    own = pltpu.make_async_copy(pool_ref, pools.at[r], local_sems.at[0])
    own_note = pltpu.make_async_copy(note_ref, notes.at[r], local_sems.at[1])
    own.start()
    own_note.start()

    barrier = pltpu.get_barrier_semaphore()
    for to in (main_to, other_to, sibling):
        pl.semaphore_signal(barrier, inc=1, device_id=(d, to), device_id_type=MESH)

    def greet(i, carry):
        pl.semaphore_signal(barrier, inc=1, device_id=(peer(i), r), device_id_type=MESH)
        return carry

    lax.fori_loop(1, n_dp, greet, 0)
    own.wait()
    own_note.wait()
    hot_sum[...] = jnp.zeros_like(hot_sum)
    pl.semaphore_wait(barrier, n_dp + 2)

    def ring(big, small, big_sems, small_sems, use):
        span = big.shape[1] // 2

        def copies(source, b, to, lane, k):
            at = big.at[source, pl.ds(b * span, span)]
            n = k * 2 + b
            yield pltpu.make_async_remote_copy(
                src_ref=at,
                dst_ref=at,
                send_sem=big_sems.at[2 * lane, n],
                recv_sem=big_sems.at[2 * lane + 1, n],
                device_id=(d, to),
                device_id_type=MESH,
            )

        def note(source, to, lane, k):
            return pltpu.make_async_remote_copy(
                src_ref=small.at[source],
                dst_ref=small.at[source],
                send_sem=small_sems.at[2 * lane, k],
                recv_sem=small_sems.at[2 * lane + 1, k],
                device_id=(d, to),
                device_id_type=MESH,
            )

        def send(source, b, to, lane, k):
            if b == 0:
                note(source, to, lane, k).start()
            for copy in copies(source, b, to, lane, k):
                copy.start()

        def arrive(source, b, to, lane, k):
            if b == 0:
                note(source, to, lane, k).wait_recv()
            for copy in copies(source, b, to, lane, k):
                copy.wait_recv()

        def sent(source, b, to, lane, k):
            if b == 0:
                note(source, to, lane, k).wait_send()
            for copy in copies(source, b, to, lane, k):
                copy.wait_send()

        def step(k, carry):
            from_main = row_of(z - sign * k, c)
            from_other = row_of(z + sign * k, c)
            has_other = jnp.logical_and(k >= 1, k <= other_hops)
            for b in range(2):

                @pl.when(k >= 1)
                def _():
                    arrive(from_main, b, main_to, 0, k - 1)

                @pl.when(k < main_hops)
                def _():
                    send(from_main, b, main_to, 0, k)

                @pl.when(has_other)
                def _():
                    arrive(from_other, b, other_to, 1, k - 1)

                @pl.when(k < other_hops)
                def _():
                    send(from_other, b, other_to, 1, k)

                send(from_main, b, sibling, 2, k)

                @pl.when(has_other)
                def _():
                    send(from_other, b, sibling, 2, main_hops + k)

                if use is None:
                    continue

                def turn(q, inner):
                    live = jnp.logical_or(q % 2 == 0, has_other)

                    @pl.when(live)
                    def _():
                        there = jnp.where(
                            jnp.logical_or(q == 0, q == 3), from_main // 2, from_other // 2
                        )
                        source = there * 2 + jnp.where(q < 2, c, 1 - c)

                        @pl.when(q >= 2)
                        def _():
                            arrive(source, b, sibling, 2, k + jnp.where(q == 3, main_hops, 0))

                        use(source, b)

                    return inner

                lax.fori_loop(0, 4, turn, 0)
            return carry

        lax.fori_loop(0, main_hops + 1, step, 0)

        for k in range(main_hops):
            for b in range(2):
                sent(r, b, main_to, 0, k)
        for k in range(other_hops):
            for b in range(2):
                sent(r, b, other_to, 1, k)
        for k in range(main_hops + 1 + other_hops):
            for b in range(2):
                sent(r, b, sibling, 2, k)
                if use is None:
                    arrive(r, b, sibling, 2, k)

    rows_at = lax.broadcasted_iota(I32, (8, 128), 0)
    hot_first = n_row * slots + r * block
    cold_first = r * slots
    low = block // 8
    cold_low = slots // 8
    groups = low // 16

    def count(source, b):
        def tile(t, carry):
            first = pl.multiple_of(t * 128, 128)
            high, field = [], []
            for j in range(16):
                word = jnp.broadcast_to(notes[source, j : j + 1, pl.ds(first, 128)], (8, 128))
                value = word & 0xFFFF if b == 0 else lax.shift_right_logical(word, 16)
                hot = value - hot_first
                cold = value - cold_first
                is_hot = jnp.logical_and(hot >= 0, hot < block)
                is_cold = jnp.logical_and(cold >= 0, cold < slots)
                top = jnp.where(is_cold, cold // cold_low, lax.shift_right_logical(hot, low.bit_length() - 1) & 7)
                high.append(
                    jnp.where(is_cold, low + (cold & (cold_low - 1)), hot & (low - 1)) - rows_at
                )
                field.append(
                    jnp.where(
                        jnp.logical_or(is_hot, is_cold),
                        lax.shift_left(jnp.ones_like(top), (top & 7) * 4),
                        0,
                    )
                )
            for k in range(groups + 1):
                parts = []
                for h in range(2):
                    base = (k * 2 + h) * 8
                    sums = []
                    for g in range(2):
                        total = jnp.zeros((8, 128), I32)
                        for j in range(8 * g, 8 * g + 8):
                            total = total + jnp.where(high[j] == base, field[j], 0)
                        sums.append(total)
                    even = (sums[0] & NIBBLES) + (sums[1] & NIBBLES)
                    odd = (lax.shift_right_logical(sums[0], 4) & NIBBLES) + (
                        lax.shift_right_logical(sums[1], 4) & NIBBLES
                    )
                    parts.append((even, odd))
                for f in range(8):
                    found = []
                    for h in range(2):
                        x = lax.shift_right_logical(parts[h][f & 1], 8 * (f >> 1))
                        found.append((x & 255).astype(F32))
                    row = f * low + k * 16 if k < groups else block + f * 16
                    tally[pl.ds(row, 16), pl.ds(first, 128)] = jnp.concatenate(found, 0).astype(BF16)
            return carry

        lax.fori_loop(0, half // 128, tile, 0)
        rows = pools[source, pl.ds(b * half, half), :]
        hot_sum[...] += jnp.dot(tally[:block, :], rows, preferred_element_type=F32)
        cold = jnp.dot(tally[block:, :], rows, preferred_element_type=F32)
        if b == 0:
            cold_out[source] = cold
        else:
            cold_out[source] += cold
            cold_in[d, source] = cold_out[source, pl.ds(pl.multiple_of(d * CAP, CAP), CAP), :]
            held = notes[source, :, half:]
            wanted = lax.broadcasted_iota(I32, held.shape, 0) == r
            ids_out[source] = jnp.sum(jnp.where(wanted, held, 0), axis=0)

            def give(i, carry):
                to = peer(i)
                pltpu.make_async_remote_copy(
                    src_ref=cold_out.at[source, pl.ds(pl.multiple_of(to * CAP, CAP), CAP)],
                    dst_ref=cold_in.at[d, source],
                    send_sem=bulk_sems.at[0],
                    recv_sem=bulk_sems.at[1],
                    device_id=(to, r),
                    device_id_type=MESH,
                ).start()
                return carry

            lax.fori_loop(1, n_dp, give, 0)

    ring(pools, notes, pool_sems, note_sems, count)

    def to_all(make):
        def go(i, carry):
            make(peer(i)).start()
            return carry

        lax.fori_loop(1, n_dp, go, 0)

    def to_dp(src, dst, n):
        def make(to):
            return pltpu.make_async_remote_copy(
                src_ref=src(to),
                dst_ref=dst,
                send_sem=bulk_sems.at[n],
                recv_sem=bulk_sems.at[n + 1],
                device_id=(to, r),
                device_id_type=MESH,
            )

        return make

    def all_bytes(ref, n):
        return pltpu.make_async_remote_copy(
            src_ref=ref,
            dst_ref=ref,
            send_sem=bulk_sems.at[n],
            recv_sem=bulk_sems.at[n + 1],
            device_id=(peer(1), r),
            device_id_type=MESH,
        )

    others = pl.ds(0, n_dp - 1)
    to_all(
        to_dp(
            lambda to: hot_sum.at[pl.ds(pl.multiple_of(to * piece, piece), piece)], hot_in.at[d], 2
        )
    )
    ids_in[d] = ids_out[...]
    to_all(to_dp(lambda to: ids_out, ids_in.at[d], 4))
    mine = pl.ds(pl.multiple_of(d * piece, piece), piece)
    hot_in[d] = hot_sum[mine, :]
    all_bytes(hot_in.at[others], 2).wait_recv()
    grad = hot_in[0]
    for k in range(1, n_dp):
        grad = grad + hot_in[k]
    per_line = 128 // piece
    line_at = pl.ds(d // per_line, 1)
    first = lax.rem(d, per_line) * piece
    update, new_m, new_s, new_scale_m, new_scale_s = adam_parts(
        codes_m_ref[mine, :],
        codes_s_ref[mine, :],
        lanes_to_column(scale_m_ref[line_at, :], piece, first),
        lanes_to_column(scale_s_ref[line_at, :], piece, first),
        grad,
    )
    widest = jnp.maximum(jnp.max(jnp.abs(update), axis=1, keepdims=True), 1e-20)
    steps_q[r, mine, :] = jnp.round(update * (32767.0 / widest)).astype(I32).astype(jnp.int16)
    line_out[0:1, :] = column_to_lanes(new_scale_m, 128)
    line_out[1:2, :] = column_to_lanes(new_scale_s, 128)
    line_out[2:3, :] = column_to_lanes(widest / 32767.0, 128)
    line_out[3:8, :] = jnp.zeros((5, 128), F32)
    new_m_ref[mine, :] = new_m
    new_s_ref[mine, :] = new_s
    lines_ref[d] = line_out[...]
    to_all(to_dp(lambda to: line_out, lines_ref.at[d], 6))
    to_all(to_dp(lambda to: steps_q.at[r, mine], steps_q.at[r, mine], 8))
    to_all(to_dp(lambda to: new_m_ref.at[mine], new_m_ref.at[mine], 10))
    to_all(to_dp(lambda to: new_s_ref.at[mine], new_s_ref.at[mine], 12))
    all_bytes(lines_ref.at[others], 6).wait_recv()
    for k in range(n_dp):
        steps_scale[r, k : k + 1, :] = lines_ref[k, 2:3, :]
    rest = pl.ds(0, block - piece)
    all_bytes(steps_q.at[r, rest], 8).wait_recv()

    ring(steps_q, steps_scale, step_sems, step_scale_sems, None)

    for ref, n in (
        (cold_in.at[others], 0),
        (ids_in.at[others], 4),
        (new_m_ref.at[rest], 10),
        (new_s_ref.at[rest], 12),
    ):
        all_bytes(ref, n).wait()
    for ref, n in (
        (hot_in.at[others], 2),
        (lines_ref.at[others], 6),
        (steps_q.at[r, rest], 8),
    ):
        all_bytes(ref, n).wait_send()


def cold_kernel(
    values_ref,
    ids_ref,
    lines_ref,
    table_ref,
    codes_m_ref,
    codes_s_ref,
    scale_m_ref,
    scale_s_ref,
    table_out,
    codes_m_out,
    codes_s_out,
    scale_m_out,
    scale_s_out,
    hot_scale_m_out,
    hot_scale_s_out,
    split,
    ids_line,
):
    n = pl.program_id(0)
    rows, width = table_ref.shape

    @pl.when(n == 0)
    def _():
        value = values_ref[...]
        top = value.astype(BF16)
        split[:, :width] = top
        split[:, width:] = (value - top.astype(F32)).astype(BF16)
        d = lax.axis_index("dp")
        senders, _, slots = ids_ref.shape
        for k in range(senders):
            x = ids_ref[k]
            lane = lax.broadcasted_iota(I32, x.shape, 1)
            x = jnp.where(lane // CAP == d, x, 0)
            shift = CAP
            while shift < slots:
                x = x + pltpu.roll(x, shift, 1)
                shift *= 2
            own = lane // CAP == lax.broadcasted_iota(I32, x.shape, 0)
            ids_line[0:1, k * slots : (k + 1) * slots] = jnp.sum(
                jnp.where(own, x, 0), axis=0, keepdims=True
            )
        lines = hot_scale_m_out.shape[0]
        per_line = senders // lines
        piece = 128 // per_line
        for ref, out in ((0, hot_scale_m_out), (1, hot_scale_s_out)):
            for k in range(lines):
                line = lines_ref[k * per_line, ref : ref + 1, :]
                for i in range(1, per_line):
                    line = line + pltpu.roll(lines_ref[k * per_line + i, ref : ref + 1, :], i * piece, 1)
                out[k : k + 1, :] = line

    ids = ids_line[...]
    shape = (rows, ids.shape[1])
    wanted = lax.broadcasted_iota(I32, shape, 0) + n * rows
    match = jnp.where(wanted == jnp.broadcast_to(ids, shape), 1.0, 0.0).astype(BF16)
    both = jnp.dot(match, split[...], preferred_element_type=F32)
    grad = both[:, :width] + both[:, width:]
    for k in range(rows // 128):
        at = slice(k * 128, (k + 1) * 128)
        line = pl.ds(n * (rows // 128) + k, 1)
        update, new_m, new_s, scale_m, scale_s = adam_parts(
            codes_m_ref[at, :],
            codes_s_ref[at, :],
            lanes_to_column(scale_m_ref[line, :], 128, 0),
            lanes_to_column(scale_s_ref[line, :], 128, 0),
            grad[at, :],
        )
        table_out[at, :] = table_ref[at, :] - update
        codes_m_out[at, :] = new_m
        codes_s_out[at, :] = new_s
        scale_m_out[line, :] = column_to_lanes(scale_m, 128)
        scale_s_out[line, :] = column_to_lanes(scale_s, 128)


def replica_kernel(table_ref, steps_ref, scale_ref, out_ref):
    blocks, pieces = scale_ref.shape[:2]
    block = steps_ref.shape[1]
    piece = block // pieces
    for n in range(blocks):
        for k in range(pieces):
            at = slice(n * block + k * piece, n * block + (k + 1) * piece)
            scale = lanes_to_column(scale_ref[n, k : k + 1, :], piece, 0)
            moved = steps_ref[n, k * piece : (k + 1) * piece, :].astype(I32).astype(F32)
            out_ref[at, :] = table_ref[at, :] - moved * scale


def body(
    n_dp,
    n_row,
    bag_index,
    pooled_grad,
    touched_ids,
    owner_counts,
    cold_table,
    cold_moment_codes,
    cold_second_codes,
    cold_moment_scales,
    cold_second_scales,
    hot_table,
    hot_moment_codes,
    hot_second_codes,
    hot_moment_scales,
    hot_second_scales,
):
    samples, pool = bag_index.shape
    width = pooled_grad.shape[1]
    hot_rows = hot_table.shape[0]
    own_rows = cold_table.shape[0]
    block = hot_rows // n_row
    slots = n_dp * CAP
    owners = n_dp * n_row

    vmem = pl.BlockSpec(memory_space=pltpu.VMEM)
    smem = pl.BlockSpec(memory_space=pltpu.SMEM)
    note = pl.pallas_call(
        functools.partial(note_kernel, n_dp, n_row),
        out_shape=jax.ShapeDtypeStruct((pool, samples // 2 + slots), I32),
        in_specs=[smem, smem, vmem],
        out_specs=vmem,
        compiler_params=pltpu.CompilerParams(vmem_limit_bytes=63 * 1024 * 1024),
    )(owner_counts, touched_ids, bag_index.T)

    chips = n_row // 2
    main_hops, other_hops = chips // 2, chips // 2 - 1
    flows = main_hops + 1 + other_hops
    cold_in, ids_in, steps_q, steps_scale, new_m, new_s, lines = pl.pallas_call(
        functools.partial(exchange_kernel, n_dp, n_row),
        out_shape=(
            jax.ShapeDtypeStruct((n_dp, n_row, CAP, width), F32),
            jax.ShapeDtypeStruct((n_dp, n_row, slots), I32),
            jax.ShapeDtypeStruct((n_row, block, width), jnp.int16),
            jax.ShapeDtypeStruct((n_row, n_dp, 128), F32),
            jax.ShapeDtypeStruct((block, width), BF16),
            jax.ShapeDtypeStruct((block, width), BF16),
            jax.ShapeDtypeStruct((n_dp, 8, 128), F32),
        ),
        in_specs=[vmem] * 6,
        out_specs=(vmem,) * 7,
        scratch_shapes=[
            pltpu.VMEM((n_row, samples, width), BF16),
            pltpu.VMEM((n_row, pool, samples // 2 + slots), I32),
            pltpu.VMEM((block + slots, samples // 2), BF16),
            pltpu.VMEM((block, width), F32),
            pltpu.VMEM((n_row, slots, width), F32),
            pltpu.VMEM((n_row, slots), I32),
            pltpu.VMEM((n_dp, block // n_dp, width), F32),
            pltpu.VMEM((8, 128), F32),
            pltpu.SemaphoreType.DMA((6, 2 * flows)),
            pltpu.SemaphoreType.DMA((6, flows)),
            pltpu.SemaphoreType.DMA((6, 2 * flows)),
            pltpu.SemaphoreType.DMA((6, flows)),
            pltpu.SemaphoreType.DMA((14,)),
            pltpu.SemaphoreType.DMA((2,)),
        ],
        compiler_params=pltpu.CompilerParams(
            collective_id=0, has_side_effects=True, vmem_limit_bytes=63 * 1024 * 1024
        ),
    )(
        pooled_grad,
        note,
        hot_moment_codes,
        hot_second_codes,
        hot_moment_scales.reshape(-1, 128),
        hot_second_scales.reshape(-1, 128),
    )

    hot_lines = block // 128
    whole3 = lambda a: pl.BlockSpec(a.shape, lambda n: (0, 0, 0))
    tile = own_rows // 4
    lines_of = own_rows // 128
    whole = lambda a, b: pl.BlockSpec((a, b), lambda n: (0, 0))
    rows = pl.BlockSpec((tile, width), lambda n: (n, 0))
    cold = pl.pallas_call(
        cold_kernel,
        grid=(own_rows // tile,),
        out_shape=(
            jax.ShapeDtypeStruct((own_rows, width), F32),
            jax.ShapeDtypeStruct((own_rows, width), BF16),
            jax.ShapeDtypeStruct((own_rows, width), BF16),
            jax.ShapeDtypeStruct((lines_of, 128), F32),
            jax.ShapeDtypeStruct((lines_of, 128), F32),
            jax.ShapeDtypeStruct((hot_lines, 128), F32),
            jax.ShapeDtypeStruct((hot_lines, 128), F32),
        ),
        in_specs=[
            whole(owners * CAP, width),
            whole3(ids_in),
            whole3(lines),
            rows,
            rows,
            rows,
            whole(lines_of, 128),
            whole(lines_of, 128),
        ],
        out_specs=(
            rows,
            rows,
            rows,
            whole(lines_of, 128),
            whole(lines_of, 128),
            whole(hot_lines, 128),
            whole(hot_lines, 128),
        ),
        scratch_shapes=[
            pltpu.VMEM((owners * CAP, 2 * width), BF16),
            pltpu.VMEM((1, owners * CAP), I32),
        ],
    )(
        cold_in.reshape(-1, width),
        ids_in,
        lines,
        cold_table,
        cold_moment_codes,
        cold_second_codes,
        cold_moment_scales.reshape(-1, 128),
        cold_second_scales.reshape(-1, 128),
    )
    replica = pl.pallas_call(
        replica_kernel,
        grid=(n_row // 4,),
        out_shape=jax.ShapeDtypeStruct((hot_rows, width), F32),
        in_specs=[
            pl.BlockSpec((4 * block, width), lambda n: (n, 0)),
            pl.BlockSpec((4, block, width), lambda n: (n, 0, 0)),
            pl.BlockSpec((4, n_dp, 128), lambda n: (n, 0, 0)),
        ],
        out_specs=pl.BlockSpec((4 * block, width), lambda n: (n, 0)),
    )(hot_table, steps_q, steps_scale)
    return (
        cold[0],
        cold[1],
        cold[2],
        cold[3].reshape(-1),
        cold[4].reshape(-1),
        replica,
        new_m,
        new_s,
        cold[5].reshape(-1),
        cold[6].reshape(-1),
    )


def solution(mesh):
    both = P(("dp", "row"), None)
    line = P(("dp", "row"))
    return jax.shard_map(
        functools.partial(body, mesh.shape["dp"], mesh.shape["row"]),
        mesh=mesh,
        in_specs=(
            both,
            both,
            both,
            both,
            both,
            both,
            both,
            line,
            line,
            P(),
            P("row", None),
            P("row", None),
            P("row"),
            P("row"),
        ),
        out_specs=(
            both,
            both,
            both,
            line,
            line,
            P(),
            P("row", None),
            P("row", None),
            P("row"),
            P("row"),
        ),
        check_vma=False,
    )
```
